256 devices in a mesh: gp: 256 (over z, y, x, core).
Axes of the slice: x: 4, y: 4, z: 8, core: 2. Of those that a mesh axis runs over, the one named last changes fastest.
Arguments:
- features: bfloat16 [524288, 100], P('gp')
- labels: int32 [524288], P('gp')
- train_mask: float32 [524288], P('gp')
- send_idx: int32 [65536, 8], P('gp')
- src_idx: int32 [4194304], P('gp')
- dst_idx: int32 [4194304], P('gp')
- inv_deg: float32 [524288], P('gp')
- w_self_1: bfloat16 [100, 256], replicated
- w_neigh_1: bfloat16 [100, 256], replicated
- bias_1: float32 [256], replicated
- w_self_2: bfloat16 [256, 256], replicated
- w_neigh_2: bfloat16 [256, 256], replicated
- bias_2: float32 [256], replicated
- w_self_3: bfloat16 [256, 47], replicated
- w_neigh_3: bfloat16 [256, 47], replicated
- bias_3: float32 [47], replicated
Outputs:
- output 1: float32 [], replicated
- output 2: float32 [100, 256], replicated
- output 3: float32 [100, 256], replicated
- output 4: float32 [256], replicated
- output 5: float32 [256, 256], replicated
- output 6: float32 [256, 256], replicated
- output 7: float32 [256], replicated
- output 8: float32 [256, 47], replicated
- output 9: float32 [256, 47], replicated
- output 10: float32 [47], replicated
All inputs are finite; a program needn't handle non-finite values.
Results may differ from the reference program's by a relative error of at most 0.0069051.
Values are sent between devices in bfloat16 or wider.
A program may use at most 768 MiB of HBM per device.

```python
import jax
import jax.numpy as jnp
from jax import lax

GROUP = 256
N_DEV = 2048
HALO_DEV = 2048
DEG = 8
F_IN = 100
HIDDEN = 256
CLASSES = 47
SEND = HALO_DEV // GROUP
EDGES = N_DEV * DEG
NODES = GROUP * N_DEV
TABLE_ROWS = N_DEV + HALO_DEV


def draw_graph(key):
    keys = jax.random.split(key, 8)
    send_idx = jax.random.randint(keys[0], (GROUP * GROUP, SEND), 0, N_DEV, jnp.int32)
    hub_weight = jax.random.randint(keys[1], (GROUP, 1), 1, 5, jnp.int32)
    counts = jax.random.randint(keys[2], (GROUP, GROUP), 1, SEND + 1, jnp.int32)
    counts = jnp.clip((counts * hub_weight) // 4, 1, SEND)
    dst_idx = jnp.sort(jax.random.randint(keys[3], (GROUP, EDGES), 0, N_DEV, jnp.int32), axis=1)
    from_halo = jax.random.randint(keys[4], (GROUP, EDGES), 0, 2, jnp.int32)
    local_src = jax.random.randint(keys[5], (GROUP, EDGES), 0, N_DEV, jnp.int32)
    owner = jnp.arange(GROUP, dtype=jnp.int32)[:, None]
    peer = (owner + 1 + jax.random.randint(keys[6], (GROUP, EDGES), 0, GROUP - 1, jnp.int32)) % GROUP
    slot = jax.random.randint(keys[7], (GROUP, EDGES), 0, counts[peer, owner], jnp.int32)
    src_idx = jnp.where(from_halo == 1, N_DEV + peer * SEND + slot, local_src)
    ones_row = jnp.ones((EDGES,), jnp.float32)
    degree = jax.vmap(lambda dst_row: jax.ops.segment_sum(ones_row, dst_row, num_segments=N_DEV))(dst_idx)
    inv_deg = 1.0 / jnp.maximum(degree, 1.0)
    return send_idx, src_idx.reshape(-1), dst_idx.reshape(-1), inv_deg.reshape(-1)


def draw_weight(key, fan_in, fan_out):
    normal = jax.random.normal(key, (fan_in, fan_out), jnp.float32)
    return (normal * fan_in ** -0.5).astype(jnp.bfloat16)


def setup_inputs(seed: int = 0) -> dict:
    keys = jax.random.split(jax.random.key(seed), 13)
    send_idx, src_idx, dst_idx, inv_deg = draw_graph(keys[0])
    return {
        'features': jax.random.normal(keys[1], (NODES, F_IN), jnp.float32).astype(jnp.bfloat16),
        'labels': jax.random.randint(keys[2], (NODES,), 0, CLASSES, jnp.int32),
        'train_mask': jax.random.randint(keys[3], (NODES,), 0, 2, jnp.int32).astype(jnp.float32),
        'send_idx': send_idx,
        'src_idx': src_idx,
        'dst_idx': dst_idx,
        'inv_deg': inv_deg,
        'w_self_1': draw_weight(keys[4], F_IN, HIDDEN),
        'w_neigh_1': draw_weight(keys[5], F_IN, HIDDEN),
        'bias_1': 0.5 * jax.random.normal(keys[6], (HIDDEN,), jnp.float32),
        'w_self_2': draw_weight(keys[7], HIDDEN, HIDDEN),
        'w_neigh_2': draw_weight(keys[8], HIDDEN, HIDDEN),
        'bias_2': 0.5 * jax.random.normal(keys[9], (HIDDEN,), jnp.float32),
        'w_self_3': draw_weight(keys[10], HIDDEN, CLASSES),
        'w_neigh_3': draw_weight(keys[11], HIDDEN, CLASSES),
        'bias_3': 0.5 * jax.random.normal(keys[12], (CLASSES,), jnp.float32),
    }


def reference(features, labels, train_mask, send_idx, src_idx, dst_idx, inv_deg,
              w_self_1, w_neigh_1, bias_1, w_self_2, w_neigh_2, bias_2,
              w_self_3, w_neigh_3, bias_3):
    base = jnp.arange(GROUP, dtype=jnp.int32) * N_DEV
    halo_global = (send_idx.reshape(GROUP, GROUP, SEND) + base[:, None, None]).transpose(1, 0, 2).reshape(-1)
    src_groups = src_idx.reshape(GROUP, EDGES)
    dst_groups = dst_idx.reshape(GROUP, EDGES)
    inv_groups = inv_deg.reshape(GROUP, N_DEV, 1)

    def aggregate(hidden):
        width = hidden.shape[1]
        halo = hidden[halo_global].reshape(GROUP, HALO_DEV, width)

        def one_group(pieces):
            own_rows, halo_rows, src_row, dst_row, inv_row = pieces
            table = jnp.concatenate([own_rows, halo_rows], axis=0)
            summed = jax.ops.segment_sum(table[src_row].astype(jnp.float32), dst_row, num_segments=N_DEV)
            return (summed * inv_row).astype(jnp.bfloat16)

        pieces = (hidden.reshape(GROUP, N_DEV, width), halo, src_groups, dst_groups, inv_groups)
        return lax.map(one_group, pieces).reshape(NODES, width)

    def layer(hidden, w_self, w_neigh, bias):
        neigh_mean = aggregate(hidden)
        return (jnp.dot(hidden, w_self, preferred_element_type=jnp.float32)
                + jnp.dot(neigh_mean, w_neigh, preferred_element_type=jnp.float32) + bias)

    def loss_of(params):
        hidden_1 = jax.nn.relu(layer(features, params[0], params[1], params[2])).astype(jnp.bfloat16)
        hidden_2 = jax.nn.relu(layer(hidden_1, params[3], params[4], params[5])).astype(jnp.bfloat16)
        logits = layer(hidden_2, params[6], params[7], params[8])
        log_prob = jax.nn.log_softmax(logits, axis=-1)
        picked = jnp.take_along_axis(log_prob, labels[:, None], axis=1)[:, 0]
        return jnp.sum(train_mask * -picked) / jnp.sum(train_mask)

    params = (w_self_1, w_neigh_1, bias_1, w_self_2, w_neigh_2, bias_2, w_self_3, w_neigh_3, bias_3)
    loss, grads = jax.value_and_grad(loss_of)(params)
    return (loss,
            grads[0].astype(jnp.float32), grads[1].astype(jnp.float32), grads[2].astype(jnp.float32),
            grads[3].astype(jnp.float32), grads[4].astype(jnp.float32), grads[5].astype(jnp.float32),
            grads[6].astype(jnp.float32), grads[7].astype(jnp.float32), grads[8].astype(jnp.float32))
```

```python
import functools

import jax
import jax.numpy as jnp
from jax import lax
from jax.experimental import pallas as pl
from jax.experimental.pallas import tpu as pltpu
from jax.sharding import PartitionSpec as P

AXIS = 'gp'
BF = jnp.bfloat16
F32 = jnp.float32
TILE = 256
LANES = 128
DST_TILE = 16
SRC_LO = 256
MAX_EXACT = 256
EXTRA = 128
CLS = 48

VMEM = pl.BlockSpec(memory_space=pltpu.VMEM)
SMEM = pl.BlockSpec(memory_space=pltpu.SMEM)
ANY = pl.BlockSpec(memory_space=pl.ANY)
VMEM_LIMIT = 63 * 1024 * 1024


def dot(a, b):
    return lax.dot_general(a, b, (((1,), (0,)), ((), ())), preferred_element_type=F32)


def dot_t(a, b):
    return lax.dot_general(a, b, (((1,), (1,)), ((), ())), preferred_element_type=F32)


def onehot(mask):
    return jnp.where(mask, 1.0, 0.0).astype(BF)


def rows_at(t, size=TILE):
    return pl.ds(pl.multiple_of(t * size, size), size)


def identity(size=TILE):
    return onehot(lax.broadcasted_iota(jnp.int32, (size, size), 0)
                  == lax.broadcasted_iota(jnp.int32, (size, size), 1))


def build_kernel(starts, dst_ref, src_ref, a_ref, extra_ref, pick_ref, acc_ref, count_ref):
    step = pl.program_id(0)
    tiles = a_ref.shape[0] // DST_TILE
    n_hi = a_ref.shape[1] // SRC_LO
    chunk_rows = SRC_LO // LANES

    @pl.when(step == 0)
    def _():
        pick_ref[...] = jnp.zeros_like(pick_ref)
        count_ref[0] = 0

    extra_ref[...] = jnp.zeros_like(extra_ref)

    def partial(tile, row):
        iota = lax.broadcasted_iota(jnp.int32, (n_hi * DST_TILE, LANES), 0)
        iota_lo = lax.broadcasted_iota(jnp.int32, (SRC_LO, LANES), 0)
        left, right = [], []
        for k in range(chunk_rows):
            src = src_ref[row + k]
            local = dst_ref[row + k] - tile * DST_TILE
            inside = (local >= 0) & (local < DST_TILE)
            code = jnp.where(inside, lax.shift_right_logical(src, 8) * DST_TILE + local, -1)
            left.append(onehot(iota == code))
            right.append(onehot(iota_lo == (src & (SRC_LO - 1))))
        return dot_t(jnp.concatenate(left, axis=1), jnp.concatenate(right, axis=1))

    def store(u, acc):
        out = acc.astype(BF)
        for hi in range(n_hi):
            a_ref[pl.ds(pl.multiple_of(u * DST_TILE, DST_TILE), DST_TILE), hi * SRC_LO:(hi + 1) * SRC_LO] = (
                out[hi * DST_TILE:(hi + 1) * DST_TILE])

    def one(u):
        tile = step * tiles + u
        store(u, partial(tile, starts[tile] // LANES))

    def many(u):
        tile = step * tiles + u
        first = starts[tile] // LANES
        last = starts[tile + 1]
        n_chunks = (last - first * LANES + SRC_LO - 1) // SRC_LO

        @pl.when(n_chunks > 1)
        def _():
            acc_ref[...] = jnp.zeros_like(acc_ref)

            def add(c, _):
                acc_ref[...] += partial(tile, first + c * chunk_rows)
                return 0

            lax.fori_loop(0, n_chunks, add, 0)
            store(u, acc_ref[...])

            @pl.when(last - starts[tile] > MAX_EXACT)
            def _():
                acc_ref[...] -= acc_ref[...].astype(BF).astype(F32)
                flat = (lax.broadcasted_iota(jnp.int32, acc_ref.shape, 0) * SRC_LO
                        + lax.broadcasted_iota(jnp.int32, acc_ref.shape, 1))

                def left():
                    return jnp.max(jnp.where(acc_ref[...] != 0.0, flat, -1))

                def move(at):
                    value = jnp.sum(jnp.where(flat == at, acc_ref[...], 0.0))
                    code, lo = at // SRC_LO, at % SRC_LO
                    hi, local = code // DST_TILE, code % DST_TILE
                    k = count_ref[0]
                    here = pl.ds(pl.multiple_of(u * DST_TILE, DST_TILE), DST_TILE)
                    shape = (DST_TILE, EXTRA)
                    hit = ((lax.broadcasted_iota(jnp.int32, shape, 0) == local)
                           & (lax.broadcasted_iota(jnp.int32, shape, 1) == k))
                    extra_ref[here, :] = jnp.where(hit, value, extra_ref[here, :].astype(F32)).astype(BF)
                    group = pl.ds(pl.multiple_of(k // DST_TILE * DST_TILE, DST_TILE), DST_TILE)
                    shape = (DST_TILE, pick_ref.shape[1])
                    hit = ((lax.broadcasted_iota(jnp.int32, shape, 0) == k % DST_TILE)
                           & (lax.broadcasted_iota(jnp.int32, shape, 1) == hi * SRC_LO + lo))
                    pick_ref[group, :] = jnp.where(hit, 1.0, pick_ref[group, :].astype(F32)).astype(BF)
                    count_ref[0] = k + 1
                    acc_ref[...] = jnp.where(flat == at, 0.0, acc_ref[...])
                    return left()

                lax.while_loop(lambda at: at >= 0, move, left())

    unroll = 4

    def group(g, _):
        for k in range(unroll):
            one(g * unroll + k)
        for k in range(unroll):
            many(g * unroll + k)
        return 0

    lax.fori_loop(0, tiles // unroll, group, 0)


def build_adjacency(dst_idx, src_idx, n_own, table_rows):
    edges = dst_idx.shape[0]
    tiles = n_own // DST_TILE
    bounds = jnp.arange(tiles + 1, dtype=jnp.int32) * DST_TILE
    starts = jnp.sum((dst_idx[None, :] < bounds[:, None]).astype(jnp.int32), axis=1)
    rows = edges // LANES
    pad = SRC_LO // LANES
    dst3 = jnp.pad(dst_idx.reshape(rows, 1, LANES), ((0, pad), (0, 0), (0, 0)), constant_values=-1)
    src3 = jnp.pad(src_idx.reshape(rows, 1, LANES), ((0, pad), (0, 0), (0, 0)))
    block = n_own // 8
    return pl.pallas_call(
        build_kernel,
        grid_spec=pltpu.PrefetchScalarGridSpec(
            num_scalar_prefetch=1,
            grid=(n_own // block,),
            in_specs=[pl.BlockSpec(dst3.shape, lambda i, s: (0, 0, 0)),
                      pl.BlockSpec(src3.shape, lambda i, s: (0, 0, 0))],
            out_specs=[pl.BlockSpec((block, table_rows), lambda i, s: (i, 0)),
                       pl.BlockSpec((block, EXTRA), lambda i, s: (i, 0)),
                       pl.BlockSpec((EXTRA, table_rows), lambda i, s: (0, 0))],
            scratch_shapes=[pltpu.VMEM((table_rows // SRC_LO * DST_TILE, SRC_LO), F32),
                            pltpu.SMEM((1,), jnp.int32)]),
        out_shape=[jax.ShapeDtypeStruct((n_own, table_rows), BF),
                   jax.ShapeDtypeStruct((n_own, EXTRA), BF),
                   jax.ShapeDtypeStruct((EXTRA, table_rows), BF)],
        compiler_params=pltpu.CompilerParams(vmem_limit_bytes=24 * 1024 * 1024),
        cost_estimate=pl.CostEstimate(flops=2 * edges * 2 * SRC_LO * SRC_LO, bytes_accessed=2 * n_own * table_rows,
                                      transcendentals=0),
        name='build_adjacency',
    )(starts, dst3, src3)


def load_adjacency(a_hbm, a_ref, sems):
    blocks = sems.shape[0]
    size = a_ref.shape[0] // blocks
    copies = [pltpu.make_async_copy(a_hbm.at[pl.ds(b * size, size)], a_ref.at[pl.ds(b * size, size)], sems.at[b])
              for b in range(blocks)]
    for copy in copies:
        copy.start()
    return copies


def send_rows(hidden_ref, send_col_ref, out_ref):
    n_own = hidden_ref.shape[0]

    def one(t, _):
        wanted = jnp.concatenate([send_col_ref[rows_at(t)]] * (n_own // LANES), axis=1)
        pick = onehot(wanted == lax.broadcasted_iota(jnp.int32, (TILE, n_own), 1))
        out_ref[rows_at(t)] = dot(pick, hidden_ref[...]).astype(BF)
        return 0

    lax.fori_loop(0, out_ref.shape[0] // TILE, one, 0)


def owner_sums(send_row_ref, returned_ref, t):
    n_recv = returned_ref.shape[0]
    owned = lax.broadcasted_iota(jnp.int32, (TILE, n_recv), 0) + t * TILE
    return dot(onehot(owned == send_row_ref[...]), returned_ref[...])


def aggregate(a_ref, extra_ref, table_ref, picked, inv_ref, t):
    width = table_ref.shape[1]
    total = dot(a_ref[rows_at(t)], table_ref[...]) + dot(extra_ref[rows_at(t)], picked)
    inv = inv_ref[rows_at(t)]
    if width > LANES:
        inv = jnp.concatenate([inv] * (width // LANES), axis=1)
    return (total * inv).astype(BF)


def layer_kernel(own_ref, recv_ref, a_hbm, extra_ref, pick_ref, inv_ref, send_col_ref, w_self_ref, w_neigh_ref, bias_ref,
                 h_ref, mean_ref, out_ref, a_ref, table_ref, sems):
    n_own = own_ref.shape[0]
    copies = load_adjacency(a_hbm, a_ref, sems)
    table_ref[:n_own] = own_ref[...]
    table_ref[n_own:] = recv_ref[...]
    picked = dot(pick_ref[...], table_ref[...]).astype(BF)
    for copy in copies:
        copy.wait()

    def one(t, _):
        mean = aggregate(a_ref, extra_ref, table_ref, picked, inv_ref, t)
        mean_ref[rows_at(t)] = mean
        pre = dot(own_ref[rows_at(t)], w_self_ref[...]) + dot(mean, w_neigh_ref[...]) + bias_ref[...]
        h_ref[rows_at(t)] = jnp.maximum(pre, 0.0).astype(BF)
        return 0

    lax.fori_loop(0, n_own // TILE, one, 0)
    send_rows(h_ref, send_col_ref, out_ref)


def gather_kernel(own_ref, send_col_ref, out_ref):
    send_rows(own_ref, send_col_ref, out_ref)


def column_product(left, a_ref, extra_ref, pick_ref, t):
    at = rows_at(t)
    total = dot(left, a_ref[:, at])
    rest = dot(left, extra_ref[...])
    high = rest.astype(BF)
    low = (rest - high.astype(F32)).astype(BF)
    return total + dot(high, pick_ref[:, at]) + dot(low, pick_ref[:, at])


def head_kernel(own_ref, recv_ref, a_hbm, extra_ref, pick_ref, inv_ref, inv_row_ref, label_ref, mask_ref,
                ws_ref, wn_ref, bias_ref,
                d_ref, own_grad_ref, out_ref, g_self_ref, g_neigh_ref, g_bias_ref, sums_ref,
                a_ref, table_ref, mean_ref, ws_pad, wn_pad, scaled_ref, sems):
    n_own = own_ref.shape[0]
    n_cls = ws_ref.shape[0]
    copies = load_adjacency(a_hbm, a_ref, sems)
    table_ref[:n_own] = own_ref[...]
    table_ref[n_own:] = recv_ref[...]
    picked = dot(pick_ref[...], table_ref[...]).astype(BF)
    ws_pad[...] = jnp.zeros_like(ws_pad)
    wn_pad[...] = jnp.zeros_like(wn_pad)
    ws_pad[:n_cls] = ws_ref[...].astype(F32)
    wn_pad[:n_cls] = wn_ref[...].astype(F32)
    w_self = ws_pad[...].astype(BF)
    w_neigh = wn_pad[...].astype(BF)
    sums_ref[...] = jnp.zeros_like(sums_ref)
    g_bias_ref[...] = jnp.zeros_like(g_bias_ref)
    for copy in copies:
        copy.wait()

    def one(t, _):
        mean = aggregate(a_ref, extra_ref, table_ref, picked, inv_ref, t)
        mean_ref[rows_at(t)] = mean
        at = rows_at(t)
        logits = dot_t(w_self, own_ref[at]) + dot_t(w_neigh, mean) + bias_ref[:, :1]
        cls = lax.broadcasted_iota(jnp.int32, (CLS, TILE), 0)
        logits = jnp.where(cls < n_cls, logits, -jnp.inf)
        shifted = logits - jnp.max(logits, axis=0, keepdims=True)
        exps = jnp.exp(shifted)
        total = jnp.sum(exps, axis=0, keepdims=True)
        is_label = cls == label_ref[:, at]
        picked_log = jnp.sum(jnp.where(is_label, shifted, 0.0), axis=0, keepdims=True) - jnp.log(total)
        mask = mask_ref[:, at]
        grad = (exps / total - jnp.where(is_label, 1.0, 0.0)) * mask
        for half in range(TILE // LANES):
            lanes = slice(half * LANES, (half + 1) * LANES)
            sums_ref[0:1] += -(mask * picked_log)[:, lanes]
            sums_ref[1:2] += mask[:, lanes]
            g_bias_ref[...] += grad[:, lanes]
        grad_bf = grad.astype(BF)
        d_ref[:, at] = grad_bf
        scaled_ref[:, at] = (grad_bf.astype(F32) * inv_row_ref[:, at]).astype(BF)
        return 0

    lax.fori_loop(0, n_own // TILE, one, 0)
    g_self_ref[...] = dot(d_ref[...], own_ref[...])
    g_neigh_ref[...] = dot(d_ref[...], mean_ref[...])

    def back(t, _):
        own_grad_ref[:, rows_at(t)] = column_product(scaled_ref[...], a_ref, extra_ref, pick_ref, t)
        return 0

    lax.fori_loop(0, n_own // TILE, back, 0)

    def back_recv(t, _):
        part = column_product(scaled_ref[...], a_ref, extra_ref, pick_ref, t + n_own // TILE)
        part = jnp.concatenate([part, jnp.zeros((LANES - CLS, TILE), F32)], axis=0)
        out_ref[rows_at(t)] = part.T.astype(BF)
        return 0

    lax.fori_loop(0, out_ref.shape[0] // TILE, back_recv, 0)


def middle_kernel(returned_ref, own_grad_ref, d_ref, own_ref, prev_ref, mean_ref, a_hbm, extra_ref, pick_ref, inv_row_ref,
                  send_row_ref, ws3_ref, wn3_ref, w_neigh_ref,
                  d_out_ref, own_out_ref, out_ref, g_self_ref, g_neigh_ref, g_bias_ref,
                  a_ref, scaled_ref, ws_pad, wn_pad, sems):
    n_own = own_ref.shape[0]
    width = own_ref.shape[1]
    n_cls = ws3_ref.shape[0]
    copies = load_adjacency(a_hbm, a_ref, sems)
    ws_pad[...] = jnp.zeros_like(ws_pad)
    wn_pad[...] = jnp.zeros_like(wn_pad)
    ws_pad[:n_cls] = ws3_ref[...].astype(F32)
    wn_pad[:n_cls] = wn3_ref[...].astype(F32)
    ws3 = ws_pad[...].T.astype(BF)
    wn3 = wn_pad[...].T.astype(BF)
    g_bias_ref[...] = jnp.zeros_like(g_bias_ref)
    eye = identity()

    def one(t, _):
        at = rows_at(t)
        sums = owner_sums(send_row_ref, returned_ref, t).T[:CLS]
        d_sum = (own_grad_ref[:, at] + sums).astype(BF)
        zero = jnp.zeros((LANES - CLS, TILE), F32)
        grown = jnp.concatenate([d_ref[:, at].astype(F32), zero], axis=0).astype(BF)
        d_sum = jnp.concatenate([d_sum.astype(F32), zero], axis=0).astype(BF)
        grad = dot(ws3, grown) + dot(wn3, d_sum)
        grad = jnp.where(dot_t(eye, own_ref[at]) > 0.0, grad, 0.0)
        for half in range(TILE // LANES):
            g_bias_ref[...] += grad[:, half * LANES:(half + 1) * LANES]
        d_out_ref[:, at] = grad.astype(BF)
        scaled_ref[:, at] = (dot(w_neigh_ref[...], grad.astype(BF)) * inv_row_ref[:, at]).astype(BF)
        return 0

    lax.fori_loop(0, n_own // TILE, one, 0)
    for copy in copies:
        copy.wait()

    def back_recv(t, _):
        part = column_product(scaled_ref[...], a_ref, extra_ref, pick_ref, t + n_own // TILE)
        out_ref[rows_at(t)] = part.T.astype(BF)
        return 0

    lax.fori_loop(0, out_ref.shape[0] // TILE, back_recv, 0)

    def back(t, _):
        own_out_ref[:, rows_at(t)] = column_product(scaled_ref[...], a_ref, extra_ref, pick_ref, t)
        return 0

    lax.fori_loop(0, n_own // TILE, back, 0)
    g_self_ref[...] = dot(d_out_ref[...], prev_ref[...]).T
    g_neigh_ref[...] = dot(d_out_ref[...], mean_ref[...]).T


def first_kernel(returned_ref, own_grad_ref, d_ref, own_ref, prev_ref, mean_ref, send_row_ref, w_self_ref,
                 g_self_ref, g_neigh_ref, g_bias_ref, d_out_ref):
    n_own = own_ref.shape[0]
    g_bias_ref[...] = jnp.zeros_like(g_bias_ref)
    eye = identity()

    def one(t, _):
        at = rows_at(t)
        sums = owner_sums(send_row_ref, returned_ref, t).T
        grad = dot(w_self_ref[...], d_ref[:, at]) + (own_grad_ref[:, at] + sums)
        grad = jnp.where(dot_t(eye, own_ref[at]) > 0.0, grad, 0.0)
        for half in range(TILE // LANES):
            g_bias_ref[...] += grad[:, half * LANES:(half + 1) * LANES]
        d_out_ref[:, at] = grad.astype(BF)
        return 0

    lax.fori_loop(0, n_own // TILE, one, 0)
    g_self_ref[...] = dot(d_out_ref[...], prev_ref[...]).T
    g_neigh_ref[...] = dot(d_out_ref[...], mean_ref[...]).T


def call(kernel, args, outs, scratch, name, flops, any_arg=None):
    return pl.pallas_call(
        kernel,
        in_specs=[ANY if i == any_arg else VMEM for i in range(len(args))],
        out_specs=[VMEM] * len(outs),
        out_shape=[jax.ShapeDtypeStruct(shape, dtype) for shape, dtype in outs],
        scratch_shapes=scratch,
        compiler_params=pltpu.CompilerParams(vmem_limit_bytes=VMEM_LIMIT),
        cost_estimate=pl.CostEstimate(flops=flops, bytes_accessed=16 * 2**20, transcendentals=0),
        name=name,
    )(*args)


def solution(mesh):
    parts = mesh.shape[AXIS]

    def device_step(features, labels, train_mask, send_idx, src_idx, dst_idx, inv_deg,
                    w_self_1, w_neigh_1, bias_1, w_self_2, w_neigh_2, bias_2,
                    w_self_3, w_neigh_3, bias_3):
        n_own, f_in = features.shape
        n_recv = send_idx.size
        rows = n_own + n_recv
        hid = w_self_2.shape[0]
        n_cls = w_self_3.shape[1]
        per_peer = send_idx.shape[1]
        dense = 2 * n_own * rows * hid

        def exchange(array):
            width = array.shape[1]
            moved = lax.all_to_all(array.reshape(parts, per_peer, width), AXIS, 0, 0, tiled=True)
            return moved.reshape(n_recv, width)

        send_flat = send_idx.reshape(-1)
        send_col = jnp.broadcast_to(send_flat[:, None], (n_recv, LANES))
        send_row = send_flat[None, :]
        inv_cols = jnp.broadcast_to(inv_deg[:, None], (n_own, LANES))
        inv_row = inv_deg[None, :]
        own_0 = jnp.pad(features, ((0, 0), (0, LANES - f_in)))
        w_self_1p = jnp.pad(w_self_1, ((0, LANES - f_in), (0, 0)))
        w_neigh_1p = jnp.pad(w_neigh_1, ((0, LANES - f_in), (0, 0)))
        bias_3c = jnp.broadcast_to(jnp.pad(bias_3, (0, CLS - n_cls))[:, None], (CLS, LANES))

        out_0, = call(gather_kernel, (own_0, send_col), [((n_recv, LANES), BF)], [], 'gather_features', dense // 8)
        recv_0 = exchange(out_0)
        adj, extra, pick = build_adjacency(dst_idx, src_idx, n_own, rows)

        def scratch(width):
            return [pltpu.VMEM((n_own, rows), BF), pltpu.VMEM((rows, width), BF)]

        sems = pltpu.SemaphoreType.DMA((8,))

        def layer(own, recv, w_self, w_neigh, bias, name):
            width = own.shape[1]
            return call(layer_kernel,
                        (own, recv, adj, extra, pick, inv_cols, send_col, w_self, w_neigh, bias[None, :]),
                        [((n_own, hid), BF), ((n_own, width), BF), ((n_recv, hid), BF)],
                        scratch(width) + [sems], name, dense, any_arg=2)

        hidden_1, mean_1, out_1 = layer(own_0, recv_0, w_self_1p, w_neigh_1p, bias_1, 'layer_1')
        recv_1 = exchange(out_1)
        hidden_2, mean_2, out_2 = layer(hidden_1, recv_1, w_self_2, w_neigh_2, bias_2, 'layer_2')
        recv_2 = exchange(out_2)
        d_3, own_grad_3, back_3, g_self_3, g_neigh_3, g_bias_3, sums = call(
            head_kernel,
            (hidden_2, recv_2, adj, extra, pick, inv_cols, inv_row, labels[None, :], train_mask[None, :],
             w_self_3.T, w_neigh_3.T, bias_3c),
            [((CLS, n_own), BF), ((CLS, n_own), F32), ((n_recv, LANES), BF), ((CLS, hid), F32), ((CLS, hid), F32),
             ((CLS, LANES), F32), ((8, LANES), F32)],
            scratch(hid) + [pltpu.VMEM((n_own, hid), BF), pltpu.VMEM((CLS, hid), F32), pltpu.VMEM((CLS, hid), F32),
                            pltpu.VMEM((CLS, n_own), BF), sems],
            'head', 2 * dense, any_arg=2)
        returned_3 = exchange(back_3)
        d_2, own_grad_2, back_2, g_self_2, g_neigh_2, g_bias_2 = call(
            middle_kernel,
            (returned_3, own_grad_3, d_3, hidden_2, hidden_1, mean_2, adj, extra, pick, inv_row, send_row,
             w_self_3.T, w_neigh_3.T, w_neigh_2),
            [((hid, n_own), BF), ((hid, n_own), F32), ((n_recv, hid), BF), ((hid, hid), F32), ((hid, hid), F32),
             ((hid, LANES), F32)],
            [pltpu.VMEM((n_own, rows), BF), pltpu.VMEM((hid, n_own), BF), pltpu.VMEM((LANES, hid), F32),
             pltpu.VMEM((LANES, hid), F32), sems],
            'middle', 2 * dense, any_arg=6)
        returned_2 = exchange(back_2)
        g_self_1, g_neigh_1, g_bias_1 = call(
            first_kernel,
            (returned_2, own_grad_2, d_2, hidden_1, own_0, mean_1, send_row, w_self_2),
            [((LANES, hid), F32), ((LANES, hid), F32), ((hid, LANES), F32)],
            [pltpu.VMEM((hid, n_own), BF)], 'first', dense)

        pieces = [g_self_1[:f_in], g_neigh_1[:f_in], g_self_2, g_neigh_2, g_self_3[:n_cls], g_neigh_3[:n_cls],
                  jnp.sum(g_bias_1, axis=1), jnp.sum(g_bias_2, axis=1), jnp.sum(g_bias_3, axis=1)[:n_cls],
                  jnp.sum(sums[:2], axis=1)]
        sizes = [piece.size for piece in pieces]
        slice_rows = -(-sum(sizes) // (parts * LANES))
        slice_rows = -(-slice_rows // 8) * 8
        flat = jnp.concatenate([piece.reshape(-1) for piece in pieces])
        flat = jnp.pad(flat, (0, parts * slice_rows * LANES - flat.shape[0])).reshape(parts, slice_rows, LANES)
        summed = jnp.sum(lax.all_to_all(flat, AXIS, 0, 0, tiled=True), axis=0)
        whole = lax.all_to_all(jnp.broadcast_to(summed[None], flat.shape), AXIS, 0, 0, tiled=True).reshape(-1)
        offsets = [sum(sizes[:i]) for i in range(len(sizes))]
        got = [whole[o:o + s].reshape(piece.shape) for o, s, piece in zip(offsets, sizes, pieces)]
        loss_sum, count = got[9][0], got[9][1]
        scale = 1.0 / count
        return (loss_sum / count,
                got[0] * scale, got[1] * scale, got[6] * scale,
                got[2] * scale, got[3] * scale, got[7] * scale,
                got[4].T * scale, got[5].T * scale, got[8] * scale)

    sharded = P(AXIS)
    whole = P()
    return jax.shard_map(device_step, mesh=mesh,
                         in_specs=(sharded,) * 7 + (whole,) * 9,
                         out_specs=(whole,) * 10, check_vma=False)
```
